32 devices in a mesh: dp: 16 (over z, x, core), mp: 2 (over y).
Axes of the slice: x: 2, y: 2, z: 4, core: 2. Of those that a mesh axis runs over, the one named last changes fastest.
Arguments:
- clean: bfloat16 [16, 1024, 1280], P('dp', 'mp'), may hold values from -6 to 6
- noise: bfloat16 [16, 1024, 1280], P('dp', 'mp'), may hold values from -6 to 6
- tsteps: int32 [16], P('dp'), may hold values from 0 to 999
- alpha_tab: float32 [1000], replicated, may hold values from 0.3 to 0.99
- weight_tab: float32 [1000], replicated, may hold values from 0.1 to 3
- norm1_gain: float32 [1280], replicated, may hold values from 0.1 to 1.9
- norm2_gain: float32 [1280], replicated, may hold values from 0.1 to 1.9
- wqkv: bfloat16 [3, 1280, 1280], P(None, 'dp', 'mp'), may hold values from -4 to 4
- wout: bfloat16 [1280, 1280], P('dp', 'mp'), may hold values from -0.625 to 0.625
- wgate: bfloat16 [1280, 5120], P('dp', 'mp'), may hold values from -0.15625 to 0.15625
- wvalue: bfloat16 [1280, 5120], P('dp', 'mp'), may hold values from -0.15625 to 0.15625
- wdown: bfloat16 [5120, 1280], P('mp', 'dp'), may hold values from -0.078125 to 0.078125
Outputs:
- denoised: float32 [16, 1024, 1280], P('dp', 'mp')
- loss: float32 [], replicated
The draws below stay inside these ranges and needn't reach their ends.
All inputs are finite; a program needn't handle non-finite values.
Results may differ from the reference program's by a relative error of at most 0.02.
Values may be sent and summed in bfloat16 or wider, within the bound.
No kernel may reach another device: no remote copies, remote signals or barrier semaphores. Data moves between devices by JAX's collectives and lax.ppermute only.
A program may use at most 128 MiB of HBM per device.

```python
import math
import jax
import jax.numpy as jnp
from jax import lax

D = 1280
HEADS = 20
HEAD = 64
FF = 5120
L = 1024
TSTEPS = 1000
B = 16
N_MP = 2


def draw_wqkv(key, part):
    base_key = jax.random.fold_in(key, 11)
    weights = jnp.clip(jax.random.normal(base_key, (3, D, D), jnp.float32), -4.0, 4.0) * D ** (-0.5)
    return weights.astype(jnp.bfloat16)


def plant(values, stream_key, least, top_value):
    index_at = [jax.random.randint(jax.random.fold_in(stream_key, axis), (), 0, length) for axis, length in enumerate(values.shape)]
    widest = values.shape.index(max(values.shape))
    neighbour = index_at[:widest] + [(index_at[widest] + 1) % values.shape[widest]] + index_at[widest + 1:]
    return values.at[tuple(index_at)].set(least).at[tuple(neighbour)].set(top_value)


def block_levels(key, extent, shards, least, high):
    level = 1.0
    for position, blocks in shards:
        steps = jax.random.uniform(jax.random.fold_in(jax.random.fold_in(key, 6), position), (blocks,), jnp.float32, least / len(shards), high / len(shards))
        level = level * jnp.repeat(jnp.exp(steps), extent[position] // blocks).reshape((-1,) + (1,) * (len(extent) - 1 - position))
    return level


def gaussian(key, shape, deviation, limit, cuts=(), kind=jnp.bfloat16):
    array = deviation * jax.random.normal(key, shape, jnp.float32)
    if cuts:
        array = array * block_levels(key, shape, cuts, -0.22, 0.18)
    return jnp.clip(array, -limit, limit).astype(kind)


def setup_inputs(seed: int = 0) -> dict:
    streams_of = jax.random.split(jax.random.key(seed), 13)
    clean = gaussian(streams_of[0], (B, L, D), 1.0, 6.0, ((0, 16), (1, 2)))
    noise = gaussian(streams_of[1], (B, L, D), 1.0, 6.0, ((0, 16), (1, 2)))
    tsteps = plant(jax.random.randint(streams_of[2], (B,), 0, TSTEPS), jax.random.fold_in(streams_of[2], 1), 0, TSTEPS - 1).astype(jnp.int32)
    alpha_tab = jnp.clip(jnp.exp(jax.random.uniform(streams_of[3], (TSTEPS,), jnp.float32, math.log(0.3), math.log(0.99))), 0.3, 0.99)
    weight_tab = jnp.clip(jnp.exp(jax.random.uniform(streams_of[4], (TSTEPS,), jnp.float32, math.log(0.1), math.log(3.0))), 0.1, 3.0)
    norm1_gain = jnp.clip(1.0 + 0.18 * jax.random.normal(streams_of[5], (D,), jnp.float32), 0.1, 1.9)
    norm2_gain = jnp.clip(1.0 + 0.18 * jax.random.normal(streams_of[6], (D,), jnp.float32), 0.1, 1.9)
    wqkv = draw_wqkv(jax.random.fold_in(streams_of[12], 71), 0)
    wout = gaussian(streams_of[8], (D, D), (D // 16) ** -0.5, 0.625, ((0, 16), (1, 2)))
    wgate = gaussian(streams_of[9], (D, FF), D ** -0.5, 0.15625, ((0, 16), (1, 2)))
    wvalue = gaussian(streams_of[10], (D, FF), D ** -0.5, 0.15625, ((0, 16), (1, 2)))
    wdown = gaussian(streams_of[11], (FF, D), FF ** -0.5, 0.078125, ((0, 2), (1, 16)))
    return dict(clean=clean, noise=noise, tsteps=tsteps, alpha_tab=alpha_tab, weight_tab=weight_tab, norm1_gain=norm1_gain, norm2_gain=norm2_gain, wqkv=wqkv, wout=wout, wgate=wgate, wvalue=wvalue, wdown=wdown)


def lookup(steps, table):
    match = steps[:, None] == jnp.arange(table.shape[0], dtype=jnp.int32)[None, :]
    return lax.optimization_barrier(jnp.sum(jnp.where(match, table[None, :], jnp.zeros((), table.dtype)), axis=1))

def layer_norm(values, gain):
    wide = values.astype(jnp.float32)
    center = wide - lax.optimization_barrier(jnp.mean(wide, axis=-1, keepdims=True))
    spread = lax.optimization_barrier(jnp.mean(center * center, axis=-1, keepdims=True))
    return (center * lax.rsqrt(spread + 1e-05) * gain).astype(jnp.bfloat16)

def one_sample(noised_one, norm1_gain, norm2_gain, wqkv, wout, wgate, wvalue, wdown):
    normed1 = layer_norm(noised_one, norm1_gain)
    query = jnp.dot(normed1, wqkv[0], preferred_element_type=jnp.float32).astype(jnp.bfloat16)
    keys = jnp.dot(normed1, wqkv[1], preferred_element_type=jnp.float32).astype(jnp.bfloat16)
    values = jnp.dot(normed1, wqkv[2], preferred_element_type=jnp.float32).astype(jnp.bfloat16)
    q_heads = query.reshape(L, HEADS, HEAD).astype(jnp.float32)
    k_heads = keys.reshape(L, HEADS, HEAD).astype(jnp.float32)
    v_heads = values.reshape(L, HEADS, HEAD).astype(jnp.float32)
    scores = jnp.einsum('qhd,khd->hqk', q_heads, k_heads) * HEAD ** (-0.5)
    probs = jax.nn.softmax(scores, axis=-1).astype(jnp.bfloat16)
    mixed = jnp.einsum('hqk,khd->qhd', probs.astype(jnp.float32), v_heads).astype(jnp.bfloat16).reshape(L, D)
    resid = (noised_one.astype(jnp.float32) + jnp.dot(mixed, wout, preferred_element_type=jnp.float32)).astype(jnp.bfloat16)
    normed2 = layer_norm(resid, norm2_gain)
    gate = jnp.dot(normed2, wgate, preferred_element_type=jnp.float32)
    value = jnp.dot(normed2, wvalue, preferred_element_type=jnp.float32)
    hidden = (jax.nn.gelu(gate, approximate=False) * value).astype(jnp.bfloat16)
    blocks = jnp.einsum('lkf,kfd->kld', hidden.reshape(L, N_MP, FF // N_MP).astype(jnp.float32), wdown.reshape(N_MP, FF // N_MP, D).astype(jnp.float32))
    ff_out = lax.optimization_barrier(jnp.sum(blocks.astype(jnp.bfloat16).astype(jnp.float32), axis=0))
    return resid.astype(jnp.float32) + ff_out

def reference(clean, noise, tsteps, alpha_tab, weight_tab, norm1_gain, norm2_gain, wqkv, wout, wgate, wvalue, wdown):
    alpha = lookup(tsteps, alpha_tab)
    sigma = jnp.sqrt(1.0 - alpha * alpha)
    weight = lookup(tsteps, weight_tab)
    noised = (alpha[:, None, None] * clean.astype(jnp.float32) + sigma[:, None, None] * noise.astype(jnp.float32)).astype(jnp.bfloat16)

    def step_one(noised_one):
        return one_sample(noised_one, norm1_gain, norm2_gain, wqkv, wout, wgate, wvalue, wdown)
    prediction = lax.map(step_one, noised)
    denoised = (noised.astype(jnp.float32) - sigma[:, None, None] * prediction) / alpha[:, None, None]
    error = denoised - clean.astype(jnp.float32)
    per_sample = lax.optimization_barrier(jnp.mean(error * error, axis=(1, 2)))
    return (denoised, jnp.sum(weight * per_sample))
```

```python
import functools

import jax
import jax.numpy as jnp
from jax import lax
from jax.experimental import pallas as pl
from jax.experimental.pallas import tpu as pltpu
from jax.sharding import PartitionSpec as P


HEADS = 20
EPS = 1e-05
CORES = 2
SIDE = 2
BF16 = jnp.bfloat16
F32 = jnp.float32
VMEM_LIMIT = 24 * 1024 * 1024


def lookup(steps, table):
    match = steps[:, None] == jnp.arange(table.shape[0], dtype=jnp.int32)[None, :]
    return jnp.sum(jnp.where(match, table[None, :], jnp.zeros((), table.dtype)), axis=1)


def layer_norm(values, gain):
    wide = values.astype(F32)
    center = wide - jnp.mean(wide, axis=-1, keepdims=True)
    spread = jnp.mean(center * center, axis=-1, keepdims=True)
    return (center * lax.rsqrt(spread + EPS) * gain).astype(BF16)


def dot(a, b):
    return jnp.dot(a, b, preferred_element_type=F32)


def dot_nt(a, b):
    return lax.dot_general(a, b, (((1,), (1,)), ((), ())), preferred_element_type=F32)


def hbm_spec():
    return pl.BlockSpec(memory_space=pltpu.HBM)


def vmem_spec():
    return pl.BlockSpec(memory_space=pltpu.VMEM)


def smem_spec():
    return pl.BlockSpec(memory_space=pltpu.SMEM)


def call(body, outs, in_specs, scratch, flops, nbytes, trans=0, out_specs=None):
    return pl.pallas_call(
        body,
        out_shape=outs,
        in_specs=in_specs,
        out_specs=out_specs if out_specs is not None else [vmem_spec() for _ in outs],
        scratch_shapes=scratch,
        compiler_params=pltpu.CompilerParams(vmem_limit_bytes=VMEM_LIMIT),
        cost_estimate=pl.CostEstimate(flops=flops, bytes_accessed=nbytes, transcendentals=trans),
    )


def piece_base(place, index, lines, rows):
    z, x = place[0], place[1]
    base = ((z ^ (index % lines)) * SIDE + (x ^ (index // lines))) * rows
    return pl.multiple_of(base, rows)


def attend_heads(q, k_ref, v_ref, pair, lane_low):
    k2 = k_ref[pair]
    v2 = v_ref[pair]
    halves = []
    for first in (True, False):
        keep = lane_low if first else jnp.logical_not(lane_low)
        qh = jnp.where(keep, q, jnp.zeros_like(q))
        s = dot_nt(qh, k2)
        m = jnp.max(s, axis=-1, keepdims=True)
        e = jnp.exp(s - m)
        total = jnp.sum(e, axis=-1, keepdims=True)
        o = dot(e.astype(BF16), v2)
        halves.append(o * (1.0 / total))
    return jnp.where(lane_low, halves[0], halves[1]).astype(BF16)


def attention_loop(q_ref, q_base, rows, k_ref, v_ref, out_ref, block):
    pairs = k_ref.shape[0]
    lane = lax.broadcasted_iota(jnp.int32, (block, 2 * HEAD_LANES), 1)
    lane_low = lane < HEAD_LANES

    def step(pair, carry):
        for t in range(rows // block):
            q = q_ref[pair, pl.ds(q_base + t * block, block), :]
            mixed = attend_heads(q, k_ref, v_ref, pair, lane_low)
            out_ref[pair, pl.ds(t * block, block), :] = mixed
        return carry

    lax.fori_loop(0, pairs, step, 0)


HEAD_LANES = 64


def qkv_body(scale, lines, place, n_own, n_peer, *refs):
    q_own, q_peer, k_out, v_out, w, sems = refs[4:]
    rows = refs[0].shape[1]
    copies = []
    for number, ref in enumerate(refs[:4]):
        slot = (place[2] ^ (number // 2)) * 2 + number % 2
        for index in range(ref.shape[0]):
            base = pl.ds(piece_base(place, index, lines, rows), rows)
            copies.append(pltpu.make_async_copy(ref.at[index], w.at[slot, base, :], sems.at[number // 2]))
    for cp in copies:
        cp.start()
    for cp in copies:
        cp.wait()
    half = n_own.shape[0]
    block = 256
    pairs = k_out.shape[0]
    for which, src in enumerate((n_own, n_peer)):
        for t in range(half // block):
            a = src[t * block : (t + 1) * block, :]
            lo = t * block
            for mat in range(3):
                r = dot(a, w[mat]).astype(BF16)
                if mat == 0:
                    r = r * jnp.asarray(scale, BF16)
                for p in range(pairs):
                    col = r[:, p * 128 : (p + 1) * 128]
                    if mat == 0:
                        (q_own, q_peer)[which][p, lo : lo + block, :] = col
                    else:
                        at = which * half + lo
                        (k_out, v_out)[mat - 1][p, at : at + block, :] = col


def attn_body(q_ref, k_ref, v_ref, mixed_ref):
    attention_loop(q_ref, 0, q_ref.shape[1], k_ref, v_ref, mixed_ref, 256)


def wout_body(lines, place, gain, noised, m_own, m_peer, packed, second, y_own, y_partner, resid_ref, n2_ref, w, sems):
    rows = packed.shape[1]
    c = place[2]

    def run(sources, act):
        for index in range(packed.shape[0]):
            base = pl.ds(piece_base(place, index, lines, rows), rows)
            for slot, ref in enumerate(sources):
                act(pltpu.make_async_copy(ref.at[index], w.at[slot, base, :], sems.at[slot]))

    for act in (lambda cp: cp.start(), lambda cp: cp.wait()):

        @pl.when(c == 1)
        def _():
            run((packed, y_own), act)

        @pl.when(c == 0)
        def _():
            run((second, y_partner), act)

    y = place[3]
    pairs = m_own.shape[0]
    width = pairs * 128
    block = 256
    own0 = pl.multiple_of(y * width, width)
    peer0 = pl.multiple_of((1 - y) * width, width)
    for t in range(noised.shape[0] // block):
        sl = slice(t * block, (t + 1) * block)
        a_own = jnp.concatenate([m_own[p, sl, :] for p in range(pairs)], axis=-1)
        a_peer = jnp.concatenate([m_peer[p, sl, :] for p in range(pairs)], axis=-1)
        outs = []
        for h in range(2):
            outs.append(dot(a_own, w[h, pl.ds(own0, width), :]) + dot(a_peer, w[h, pl.ds(peer0, width), :]))
        first = jnp.where(y == 0, outs[0], outs[1])
        second = jnp.where(y == 0, outs[1], outs[0])
        out = jnp.concatenate([first, second], axis=-1)
        r = (noised[sl, :].astype(F32) + out).astype(BF16)
        resid_ref[sl, :] = r
        n2_ref[sl, :] = layer_norm(r, gain[...])


def ff_body(has_acc, groups, lines, place, x_ref, *refs):
    half = len(groups)
    stacks, rest = (refs[:half], refs[half : 2 * half]), refs[2 * half :]
    acc_in = None
    if has_acc:
        acc_in, rest = rest[0], rest[1:]
    *outs, w, sems = rest
    acc = outs.pop() if len(outs) == 2 else outs[0]
    rows = refs[0].shape[2]
    sub = w.shape[-1]
    n_sub = refs[0].shape[-1] // sub

    def each(c_flip, s, act):
        slot = c_flip * n_sub + s
        cols = pl.ds(pl.multiple_of(s * sub, sub), sub)
        for group, ref in zip(groups, stacks[c_flip]):
            for k, index in enumerate(group):
                base = pl.ds(piece_base(place, index, lines, rows), rows)
                act(pltpu.make_async_copy(ref.at[k, :, :, cols], w.at[slot, :, base, :], sems.at[slot]))

    for s in range(n_sub):
        each(0, s, lambda cp: cp.start())

    def product(slot):
        x = x_ref[...]
        gate = dot(x, w[slot, 0])
        value = dot(x, w[slot, 1])
        hidden = (0.5 * gate * (1.0 + lax.erf(gate * (0.5**0.5))) * value).astype(BF16)
        return dot_nt(hidden, w[slot, 2])

    if has_acc:
        acc[...] = acc_in[...]
    else:
        acc[...] = jnp.zeros_like(acc)
    for c_flip in range(CORES):

        def step(s, carry):
            if c_flip == 0:
                each(1, s, lambda cp: cp.start())
            each(c_flip, s, lambda cp: cp.wait())
            acc[...] += product(c_flip * n_sub + s)
            return carry

        lax.fori_loop(0, n_sub, step, 0)
    if outs and outs[0] is not acc:
        outs[0][...] = acc[...].astype(outs[0].dtype)


def fast_shards(dp, chunks, clean, noise, tsteps, alpha_tab, weight_tab, gain1, gain2, wqkv, wout, wgate, wvalue, wdown):
    _, rows, width = clean.shape
    heads_width = wout.shape[1]
    pairs = heads_width // 128
    lines = dp // (SIDE * CORES)
    me = lax.axis_index("dp")
    y = lax.axis_index("mp")
    c = me % CORES
    x = (me // CORES) % SIDE
    z = me // (CORES * SIDE)
    place = jnp.stack([z, x, c, y]).astype(jnp.int32)
    gain_row = gain2.reshape(1, width)

    def flip(value, bits):
        return lax.ppermute(value, "dp", [(i, i ^ bits) for i in range(dp)])

    def flip_y(value):
        return lax.ppermute(value, "mp", [(0, 1), (1, 0)])

    CORE, XBIT, ZUNIT = 1, CORES, CORES * SIDE

    b0 = jnp.concatenate([wqkv, wout[None]], axis=0)
    keep0 = lax.dynamic_slice_in_dim(b0, 2 * c, 2, 0)
    give0 = lax.dynamic_slice_in_dim(b0, 2 * (1 - c), 2, 0)
    first = c == 0

    def by_core(keep, recv):
        return jnp.concatenate([jnp.where(first, keep, recv), jnp.where(first, recv, keep)], axis=1)

    own0 = by_core(keep0, flip(give0, CORE))

    alpha = lookup(tsteps, alpha_tab)
    sigma = jnp.sqrt(1.0 - alpha * alpha)
    weight = lookup(tsteps, weight_tab)
    noised = (alpha[0] * clean[0].astype(F32) + sigma[0] * noise[0].astype(F32)).astype(BF16)
    n1 = layer_norm(noised, gain1)
    n1_peer = flip_y(n1)

    ffw = jnp.stack([wgate, wvalue, wdown.T])
    hidden_half = ffw.shape[2] // CORES
    keep_f = lax.dynamic_slice_in_dim(ffw, c * hidden_half, hidden_half, 2)
    give_f = lax.dynamic_slice_in_dim(ffw, (1 - c) * hidden_half, hidden_half, 2)
    recv_f = flip(give_f, CORE)

    def gather(own, late_by_z):
        zs, xs = [own], []
        for k in range(1, lines):
            top = 1 << (k.bit_length() - 1)
            if k == top:
                zs.append(flip(own, ZUNIT * k))
            else:
                zs.append(flip(zs[top], ZUNIT * (k - top)))
        for k in range(lines):
            top = 1 << max(k.bit_length() - 1, 0)
            if late_by_z and k == lines - 1 and k != top:
                xs.append(flip(xs[top], ZUNIT * (k - top)))
            else:
                xs.append(flip(zs[k], XBIT))
        return zs, xs

    def swap_packed(parts):
        packed = jnp.stack(parts)
        return packed, flip(packed, CORE)

    zs0, xs0 = gather(own0, False)
    mats = [swap_packed([p[m] for p in zs0 + xs0]) for m in range(2)]
    packed0, second0 = mats[1]

    half_shape = jax.ShapeDtypeStruct((pairs, rows, 128), BF16)
    full_shape = jax.ShapeDtypeStruct((pairs, 2 * rows, 128), BF16)
    wbytes = 4 * width * heads_width * 2
    scale = HEAD_LANES ** (-0.5)
    q_own, q_peer, k_all, v_all = call(
        functools.partial(qkv_body, scale, lines),
        [half_shape, half_shape, full_shape, full_shape],
        [smem_spec(), vmem_spec(), vmem_spec()] + [hbm_spec()] * 4,
        [
            pltpu.VMEM((4, width, heads_width), BF16),
            pltpu.SemaphoreType.DMA((2,)),
        ],
        8 * 10**9,
        wbytes + 8 * rows * width,
    )(place, n1, n1_peer, mats[0][0], packed0, mats[0][1], second0)

    def attend(q):
        return call(
            attn_body, [half_shape], [vmem_spec()] * 3, [], 12 * 10**9, 8 * rows * width
        )(q, k_all, v_all)[0]

    mixed_peer = attend(q_peer)
    m_recv = flip_y(mixed_peer)
    mixed_own = attend(q_own)

    y_own = lax.ppermute(
        packed0, ("dp", "mp"), [(2 * i + j, 2 * i + 1 - j) for i in range(1, dp, CORES) for j in range(2)]
    )
    y_partner = lax.ppermute(y_own, "dp", [(i, i - 1) for i in range(1, dp, CORES)])
    resid, n2 = call(
        functools.partial(wout_body, lines),
        [jax.ShapeDtypeStruct((rows, width), BF16)] * 2,
        [smem_spec()] + [vmem_spec()] * 4 + [hbm_spec()] * 4,
        [pltpu.VMEM((2, width, heads_width), BF16), pltpu.SemaphoreType.DMA((2,))],
        4 * 10**9,
        wbytes,
    )(place, gain_row, noised, mixed_own, m_recv, packed0, second0, y_own, y_partner)
    n2_peer = flip_y(n2)

    def ff(tokens, groups, stacks, hc, sub, acc, out_dtype):
        n_sub = hc // sub
        t = tokens.shape[0]
        args = [place, tokens, *stacks]
        specs = [smem_spec(), vmem_spec()] + [hbm_spec()] * len(stacks)
        if acc is not None:
            args.append(acc)
            specs.append(vmem_spec())
        return call(
            functools.partial(ff_body, acc is not None, groups, lines),
            [jax.ShapeDtypeStruct((t, width), out_dtype)],
            specs,
            ([pltpu.VMEM((t, width), F32)] if out_dtype != F32 else [])
            + [
                pltpu.VMEM((CORES * n_sub, 3, width, sub), BF16),
                pltpu.SemaphoreType.DMA((CORES * n_sub,)),
            ],
            2 * t * width * hc * 2 * 3,
            3 * width * hc * 4,
        )(*args)[0]

    peer_acc = own_acc = None
    start = 0
    for index, hc in enumerate(chunks):
        sub = 256 if hc % 256 == 0 else 128
        part = slice(start, start + hc)
        zs, xs = gather(by_core(keep_f[:, :, part], recv_f[:, :, part]), index > 0)
        pieces = zs + xs
        groups = [tuple(range(lines)), tuple(range(lines, 2 * lines, 2))]
        groups += [(n,) for n in range(lines + 1, 2 * lines, 2)]
        stacks = []
        for group in groups:
            if len(group) > 1:
                stacks.append(swap_packed([pieces[n] for n in group]))
            else:
                piece = pieces[group[0]]
                stacks.append((piece[None], flip(piece, CORE)[None]))
        stacks = [pair[n] for n in range(2) for pair in stacks]
        last = index == len(chunks) - 1
        peer_acc = ff(n2_peer, groups, stacks, hc, sub, peer_acc, BF16 if last else F32)
        own_acc = ff(n2, groups, stacks, hc, sub, own_acc, F32)
        start += hc
    recv = flip_y(peer_acc)

    ratio = sigma[0] / alpha[0]
    base = noised.astype(F32) / alpha[0] - ratio * (resid.astype(F32) + own_acc)
    base = lax.optimization_barrier(base)
    denoised = base - ratio * recv.astype(F32)
    error = denoised - clean[0].astype(F32)
    total = jnp.sum(error * error) * weight[0] / (2 * rows * width)

    term = jnp.full((8, 128), total, F32)
    term = term + flip(term, CORE)
    plane = [term, flip(term, XBIT), flip_y(term)]
    corner = lax.ppermute(
        term, ("dp", "mp"), [(2 * i + j, 2 * (i ^ XBIT) + (1 - j)) for i in range(dp) for j in range(2)]
    )
    term = (plane[0] + plane[1]) + (plane[2] + corner)
    line = [term] + [flip(term, ZUNIT * k) for k in range(1, lines)]
    loss = functools.reduce(jnp.add, line)[0, 0]
    return denoised[None], loss


def make_adder(flat, piece):
    return jnp.einsum("rn,tnc->trc", flat, piece, preferred_element_type=jnp.float32)


def attend(operands):
    query_one, keys_one, values_one = operands
    rows = query_one.shape[0]
    total = keys_one.shape[0]
    scores = jnp.einsum(
        "qhd,khd->hqk",
        query_one.reshape(rows, HEADS, -1),
        keys_one.reshape(total, HEADS, -1),
        preferred_element_type=jnp.float32,
    ) * (query_one.shape[1] // HEADS) ** (-0.5)
    probs = jax.nn.softmax(scores, axis=-1).astype(jnp.bfloat16)
    mixed = jnp.einsum(
        "hqk,khd->qhd",
        probs,
        values_one.reshape(total, HEADS, -1),
        preferred_element_type=jnp.float32,
    )
    return mixed.astype(jnp.bfloat16).reshape(query_one.shape)


def plain_shards(
    clean,
    noise,
    tsteps,
    alpha_tab,
    weight_tab,
    norm1_gain,
    norm2_gain,
    wqkv,
    wout,
    wgate,
    wvalue,
    wdown,
):
    samples, local_rows, width = clean.shape
    alpha = lookup(tsteps, alpha_tab)
    sigma = jnp.sqrt(1.0 - alpha * alpha)
    weight = lookup(tsteps, weight_tab)
    noised = (
        alpha[:, None, None] * clean.astype(jnp.float32)
        + sigma[:, None, None] * noise.astype(jnp.float32)
    ).astype(jnp.bfloat16)
    normed1 = layer_norm(noised, norm1_gain)
    full_cols = lax.all_gather(wqkv, "mp", axis=2, tiled=True)
    flat = normed1.reshape(samples * local_rows, width)
    projected = make_adder(flat, lax.all_gather(full_cols, "dp", axis=1, tiled=True)).astype(
        jnp.bfloat16
    )
    query = projected[0].reshape(samples, local_rows, width)
    keys_part = projected[1].reshape(samples, local_rows, width)
    values_part = projected[2].reshape(samples, local_rows, width)
    keys_all, values_all = (
        lax.all_gather(keys_part, "mp", axis=1, tiled=True),
        lax.all_gather(values_part, "mp", axis=1, tiled=True),
    )
    mixed = lax.map(attend, (query, keys_all, values_all))
    mixed_flat = mixed.reshape(samples * local_rows, width)
    out_cols = lax.all_gather(wout, "mp", axis=1, tiled=True)
    part = mixed_flat
    projected_out = jnp.dot(
        part, lax.all_gather(out_cols, "dp", axis=0, tiled=True), preferred_element_type=jnp.float32
    )
    resid = (noised.astype(jnp.float32) + projected_out.reshape(samples, local_rows, width)).astype(
        jnp.bfloat16
    )
    normed2 = layer_norm(resid, norm2_gain)
    ff_in = lax.all_gather(normed2, "mp", axis=1, tiled=True)
    all_rows = ff_in.shape[1]
    ff_flat = ff_in.reshape(samples * all_rows, width)
    part = ff_flat
    gate = jnp.dot(
        part, lax.all_gather(wgate, "dp", axis=0, tiled=True), preferred_element_type=jnp.float32
    )
    value = jnp.dot(
        part, lax.all_gather(wvalue, "dp", axis=0, tiled=True), preferred_element_type=jnp.float32
    )
    hidden = (jax.nn.gelu(gate, approximate=False) * value).astype(jnp.bfloat16)
    block_sum = jnp.dot(
        hidden, lax.all_gather(wdown, "dp", axis=1, tiled=True), preferred_element_type=jnp.float32
    )
    ff_out = lax.psum_scatter(
        block_sum.reshape(samples, all_rows, width).astype(jnp.bfloat16),
        "mp",
        scatter_dimension=1,
        tiled=True,
    ).astype(jnp.float32)
    prediction = resid.astype(jnp.float32) + ff_out
    denoised = (noised.astype(jnp.float32) - sigma[:, None, None] * prediction) / alpha[
        :, None, None
    ]
    error = denoised - clean.astype(jnp.float32)
    local_terms = jnp.sum(weight * jnp.sum(error * error, axis=(1, 2))) / (all_rows * width)
    loss = lax.psum(local_terms, ("dp", "mp"))
    return (denoised, loss)


def solution(mesh):
    dp, mp = mesh.shape["dp"], mesh.shape["mp"]
    spec_w = P("dp", "mp")
    in_specs = (P("dp", "mp", None), P("dp", "mp", None), P("dp"), P(), P(), P(), P())
    in_specs += (P(None, "dp", "mp"), spec_w, spec_w, spec_w, P("mp", "dp"))
    out_specs = (P("dp", "mp", None), P())
    lines = dp // (SIDE * CORES)

    def run(*args):
        clean, wgate = args[0], args[9]
        hidden = wgate.shape[1] // (mp * CORES)
        width = clean.shape[2]
        fits = (
            mp == 2
            and clean.shape[0] == dp
            and lines * SIDE * CORES == dp
            and lines & (lines - 1) == 0
            and width == HEADS * HEAD_LANES
            and (width // mp) % 128 == 0
            and hidden % 256 == 0
            and (clean.shape[1] // mp) % 256 == 0
        )
        if fits:
            first = hidden * 2 // 5 // 256 * 256

            def body(*shards):
                return fast_shards(dp, (first, hidden - first), *shards)

        else:
            body = plain_shards
        step = jax.shard_map(body, mesh=mesh, in_specs=in_specs, out_specs=out_specs, check_vma=False)
        return step(*args)

    return run
```

```python
import functools

import jax
import jax.numpy as jnp
from jax import lax
from jax.experimental import pallas as pl
from jax.experimental.pallas import tpu as pltpu
from jax.sharding import PartitionSpec as P


HEADS = 20
EPS = 1e-05
CORES = 2
SIDE = 2
BF16 = jnp.bfloat16
F32 = jnp.float32
VMEM_LIMIT = 24 * 1024 * 1024


def lookup(steps, table):
    match = steps[:, None] == jnp.arange(table.shape[0], dtype=jnp.int32)[None, :]
    return jnp.sum(jnp.where(match, table[None, :], jnp.zeros((), table.dtype)), axis=1)


def layer_norm(values, gain):
    wide = values.astype(F32)
    center = wide - jnp.mean(wide, axis=-1, keepdims=True)
    spread = jnp.mean(center * center, axis=-1, keepdims=True)
    return (center * lax.rsqrt(spread + EPS) * gain).astype(BF16)


def dot(a, b):
    return jnp.dot(a, b, preferred_element_type=F32)


def dot_nt(a, b):
    return lax.dot_general(a, b, (((1,), (1,)), ((), ())), preferred_element_type=F32)


def hbm_spec():
    return pl.BlockSpec(memory_space=pltpu.HBM)


def vmem_spec():
    return pl.BlockSpec(memory_space=pltpu.VMEM)


def smem_spec():
    return pl.BlockSpec(memory_space=pltpu.SMEM)


def call(body, outs, in_specs, scratch, flops, nbytes, trans=0, out_specs=None):
    return pl.pallas_call(
        body,
        out_shape=outs,
        in_specs=in_specs,
        out_specs=out_specs if out_specs is not None else [vmem_spec() for _ in outs],
        scratch_shapes=scratch,
        compiler_params=pltpu.CompilerParams(vmem_limit_bytes=VMEM_LIMIT),
        cost_estimate=pl.CostEstimate(flops=flops, bytes_accessed=nbytes, transcendentals=trans),
    )


def piece_base(place, index, lines, rows):
    z, x = place[0], place[1]
    base = ((z ^ (index % lines)) * SIDE + (x ^ (index // lines))) * rows
    return pl.multiple_of(base, rows)


def attend_heads(q, k_ref, v_ref, pair, lane_low):
    k2 = k_ref[pair]
    v2 = v_ref[pair]
    halves = []
    for first in (True, False):
        keep = lane_low if first else jnp.logical_not(lane_low)
        qh = jnp.where(keep, q, jnp.zeros_like(q))
        s = dot_nt(qh, k2)
        m = jnp.max(s, axis=-1, keepdims=True)
        e = jnp.exp(s - m)
        total = jnp.sum(e, axis=-1, keepdims=True)
        o = dot(e.astype(BF16), v2)
        halves.append(o * (1.0 / total))
    return jnp.where(lane_low, halves[0], halves[1]).astype(BF16)


def attention_loop(q_ref, q_base, rows, k_ref, v_ref, out_ref, block):
    pairs = k_ref.shape[0]
    lane = lax.broadcasted_iota(jnp.int32, (block, 2 * HEAD_LANES), 1)
    lane_low = lane < HEAD_LANES

    def step(pair, carry):
        for t in range(rows // block):
            q = q_ref[pair, pl.ds(q_base + t * block, block), :]
            mixed = attend_heads(q, k_ref, v_ref, pair, lane_low)
            out_ref[pair, pl.ds(t * block, block), :] = mixed
        return carry

    lax.fori_loop(0, pairs, step, 0)


HEAD_LANES = 64


def qkv_body(scale, lines, place, n_own, n_peer, *refs):
    q_own, q_peer, k_out, v_out, w, sems = refs[4:]
    rows = refs[0].shape[1]
    pieces = refs[0].shape[0]

    def each(number, slot, act):
        for index in range(pieces):
            base = pl.ds(piece_base(place, index, lines, rows), rows)
            act(pltpu.make_async_copy(refs[number].at[index], w.at[slot, base, :], sems.at[slot]))

    for mat in range(2):
        for number in (mat, mat + 2):
            slot = (place[2] ^ (number // 2)) * 2 + mat

            @pl.when(slot < 3)
            def _(number=number, slot=slot):
                each(number, slot, lambda cp: cp.start())

    half = n_own.shape[0]
    block = 256
    pairs = k_out.shape[0]
    for mat in range(3):
        each(0, mat, lambda cp: cp.wait())
        for which, src in enumerate((n_own, n_peer)):
            for t in range(half // block):
                lo = t * block
                r = dot(src[lo : lo + block, :], w[mat]).astype(BF16)
                if mat == 0:
                    r = r * jnp.asarray(scale, BF16)
                for p in range(pairs):
                    col = r[:, p * 128 : (p + 1) * 128]
                    if mat == 0:
                        (q_own, q_peer)[which][p, lo : lo + block, :] = col
                    else:
                        at = which * half + lo
                        (k_out, v_out)[mat - 1][p, at : at + block, :] = col


def attn_body(q_ref, k_ref, v_ref, mixed_ref):
    attention_loop(q_ref, 0, q_ref.shape[1], k_ref, v_ref, mixed_ref, 256)


def wout_body(lines, place, gain, noised, m_own, m_peer, packed, second, y_own, y_partner, resid_ref, n2_ref, w, sems):
    rows = packed.shape[1]
    c = place[2]

    def run(sources, act):
        for index in range(packed.shape[0]):
            base = pl.ds(piece_base(place, index, lines, rows), rows)
            for slot, ref in enumerate(sources):
                act(pltpu.make_async_copy(ref.at[index], w.at[slot, base, :], sems.at[slot]))

    for act in (lambda cp: cp.start(), lambda cp: cp.wait()):

        @pl.when(c == 1)
        def _():
            run((packed, y_own), act)

        @pl.when(c == 0)
        def _():
            run((second, y_partner), act)

    y = place[3]
    pairs = m_own.shape[0]
    width = pairs * 128
    block = 256
    own0 = pl.multiple_of(y * width, width)
    peer0 = pl.multiple_of((1 - y) * width, width)
    for t in range(noised.shape[0] // block):
        sl = slice(t * block, (t + 1) * block)
        a_own = jnp.concatenate([m_own[p, sl, :] for p in range(pairs)], axis=-1)
        a_peer = jnp.concatenate([m_peer[p, sl, :] for p in range(pairs)], axis=-1)
        outs = []
        for h in range(2):
            outs.append(dot(a_own, w[h, pl.ds(own0, width), :]) + dot(a_peer, w[h, pl.ds(peer0, width), :]))
        first = jnp.where(y == 0, outs[0], outs[1])
        second = jnp.where(y == 0, outs[1], outs[0])
        out = jnp.concatenate([first, second], axis=-1)
        r = (noised[sl, :].astype(F32) + out).astype(BF16)
        resid_ref[sl, :] = r
        n2_ref[sl, :] = layer_norm(r, gain[...])


def ff_body(has_acc, groups, lines, place, x_ref, *refs):
    half = len(groups)
    stacks, rest = (refs[:half], refs[half : 2 * half]), refs[2 * half :]
    acc_in = None
    if has_acc:
        acc_in, rest = rest[0], rest[1:]
    *outs, w, sems = rest
    acc = outs.pop() if len(outs) == 2 else outs[0]
    rows = refs[0].shape[2]
    sub = w.shape[-1]
    n_sub = refs[0].shape[-1] // sub

    def each(c_flip, s, act):
        slot = c_flip * n_sub + s
        cols = pl.ds(pl.multiple_of(s * sub, sub), sub)
        for group, ref in zip(groups, stacks[c_flip]):
            for k, index in enumerate(group):
                base = pl.ds(piece_base(place, index, lines, rows), rows)
                act(pltpu.make_async_copy(ref.at[k, :, :, cols], w.at[slot, :, base, :], sems.at[slot]))

    for s in range(n_sub):
        each(0, s, lambda cp: cp.start())

    def product(slot):
        x = x_ref[...]
        gate = dot(x, w[slot, 0])
        value = dot(x, w[slot, 1])
        hidden = (0.5 * gate * (1.0 + lax.erf(gate * (0.5**0.5))) * value).astype(BF16)
        return dot_nt(hidden, w[slot, 2])

    if has_acc:
        acc[...] = acc_in[...]
    else:
        acc[...] = jnp.zeros_like(acc)
    for c_flip in range(CORES):

        def step(s, carry):
            if c_flip == 0:
                each(1, s, lambda cp: cp.start())
            each(c_flip, s, lambda cp: cp.wait())
            acc[...] += product(c_flip * n_sub + s)
            return carry

        lax.fori_loop(0, n_sub, step, 0)
    if outs and outs[0] is not acc:
        outs[0][...] = acc[...].astype(outs[0].dtype)


def fast_shards(dp, chunks, clean, noise, tsteps, alpha_tab, weight_tab, gain1, gain2, wqkv, wout, wgate, wvalue, wdown):
    _, rows, width = clean.shape
    heads_width = wout.shape[1]
    pairs = heads_width // 128
    lines = dp // (SIDE * CORES)
    me = lax.axis_index("dp")
    y = lax.axis_index("mp")
    c = me % CORES
    x = (me // CORES) % SIDE
    z = me // (CORES * SIDE)
    place = jnp.stack([z, x, c, y]).astype(jnp.int32)
    gain_row = gain2.reshape(1, width)

    def flip(value, bits):
        return lax.ppermute(value, "dp", [(i, i ^ bits) for i in range(dp)])

    def flip_y(value):
        return lax.ppermute(value, "mp", [(0, 1), (1, 0)])

    CORE, XBIT, ZUNIT = 1, CORES, CORES * SIDE

    b0 = jnp.concatenate([wqkv, wout[None]], axis=0)
    keep0 = lax.dynamic_slice_in_dim(b0, 2 * c, 2, 0)
    give0 = lax.dynamic_slice_in_dim(b0, 2 * (1 - c), 2, 0)
    first = c == 0

    def by_core(keep, recv):
        return jnp.concatenate([jnp.where(first, keep, recv), jnp.where(first, recv, keep)], axis=1)

    own0 = by_core(keep0, flip(give0, CORE))

    alpha = lookup(tsteps, alpha_tab)
    sigma = jnp.sqrt(1.0 - alpha * alpha)
    weight = lookup(tsteps, weight_tab)
    noised = (alpha[0] * clean[0].astype(F32) + sigma[0] * noise[0].astype(F32)).astype(BF16)
    n1 = layer_norm(noised, gain1)
    n1_peer = flip_y(n1)

    ffw = jnp.stack([wgate, wvalue, wdown.T])
    hidden_half = ffw.shape[2] // CORES
    keep_f = lax.dynamic_slice_in_dim(ffw, c * hidden_half, hidden_half, 2)
    give_f = lax.dynamic_slice_in_dim(ffw, (1 - c) * hidden_half, hidden_half, 2)
    recv_f = flip(give_f, CORE)

    def gather(own, late_by_z):
        zs, xs = [own], []
        for k in range(1, lines):
            top = 1 << (k.bit_length() - 1)
            if k == top:
                zs.append(flip(own, ZUNIT * k))
            else:
                zs.append(flip(zs[top], ZUNIT * (k - top)))
        for k in range(lines):
            top = 1 << max(k.bit_length() - 1, 0)
            if late_by_z and k == lines - 1 and k != top:
                xs.append(flip(xs[top], ZUNIT * (k - top)))
            else:
                xs.append(flip(zs[k], XBIT))
        return zs, xs

    def swap_packed(parts):
        packed = jnp.stack(parts)
        return packed, flip(packed, CORE)

    zs0, xs0 = gather(own0, False)
    mats = [swap_packed([p[m] for p in zs0 + xs0]) for m in range(2)]
    packed0, second0 = mats[1]

    half_shape = jax.ShapeDtypeStruct((pairs, rows, 128), BF16)
    full_shape = jax.ShapeDtypeStruct((pairs, 2 * rows, 128), BF16)
    wbytes = 4 * width * heads_width * 2
    scale = HEAD_LANES ** (-0.5)
    q_own, q_peer, k_all, v_all = call(
        functools.partial(qkv_body, scale, lines),
        [half_shape, half_shape, full_shape, full_shape],
        [smem_spec(), vmem_spec(), vmem_spec()] + [hbm_spec()] * 4,
        [
            pltpu.VMEM((3, width, heads_width), BF16),
            pltpu.SemaphoreType.DMA((3,)),
        ],
        8 * 10**9,
        wbytes + 8 * rows * width,
    )(place, n1, n1_peer, mats[0][0], packed0, mats[0][1], second0)

    def attend(q):
        return call(
            attn_body, [half_shape], [vmem_spec()] * 3, [], 12 * 10**9, 8 * rows * width
        )(q, k_all, v_all)[0]

    mixed_peer = attend(q_peer)
    m_recv = flip_y(mixed_peer)
    mixed_own = attend(q_own)

    y_own = lax.ppermute(
        packed0, ("dp", "mp"), [(2 * i + j, 2 * i + 1 - j) for i in range(1, dp, CORES) for j in range(2)]
    )
    y_partner = lax.ppermute(y_own, "dp", [(i, i - 1) for i in range(1, dp, CORES)])
    resid, n2 = call(
        functools.partial(wout_body, lines),
        [jax.ShapeDtypeStruct((rows, width), BF16)] * 2,
        [smem_spec()] + [vmem_spec()] * 4 + [hbm_spec()] * 4,
        [pltpu.VMEM((2, width, heads_width), BF16), pltpu.SemaphoreType.DMA((2,))],
        4 * 10**9,
        wbytes,
    )(place, gain_row, noised, mixed_own, m_recv, packed0, second0, y_own, y_partner)
    n2_peer = flip_y(n2)

    def ff(tokens, groups, stacks, hc, sub, acc, out_dtype):
        n_sub = hc // sub
        t = tokens.shape[0]
        args = [place, tokens, *stacks]
        specs = [smem_spec(), vmem_spec()] + [hbm_spec()] * len(stacks)
        if acc is not None:
            args.append(acc)
            specs.append(vmem_spec())
        return call(
            functools.partial(ff_body, acc is not None, groups, lines),
            [jax.ShapeDtypeStruct((t, width), out_dtype)],
            specs,
            ([pltpu.VMEM((t, width), F32)] if out_dtype != F32 else [])
            + [
                pltpu.VMEM((CORES * n_sub, 3, width, sub), BF16),
                pltpu.SemaphoreType.DMA((CORES * n_sub,)),
            ],
            2 * t * width * hc * 2 * 3,
            3 * width * hc * 4,
        )(*args)[0]

    peer_acc = own_acc = None
    start = 0
    for index, hc in enumerate(chunks):
        sub = 256 if hc % 256 == 0 else 128
        part = slice(start, start + hc)
        zs, xs = gather(by_core(keep_f[:, :, part], recv_f[:, :, part]), index > 0)
        pieces = zs + xs
        groups = [tuple(range(lines)), tuple(range(lines, 2 * lines, 2))]
        groups += [(n,) for n in range(lines + 1, 2 * lines, 2)]
        stacks = []
        for group in groups:
            if len(group) > 1:
                stacks.append(swap_packed([pieces[n] for n in group]))
            else:
                piece = pieces[group[0]]
                stacks.append((piece[None], flip(piece, CORE)[None]))
        stacks = [pair[n] for n in range(2) for pair in stacks]
        last = index == len(chunks) - 1
        peer_acc = ff(n2_peer, groups, stacks, hc, sub, peer_acc, BF16 if last else F32)
        own_acc = ff(n2, groups, stacks, hc, sub, own_acc, F32)
        start += hc
    recv = flip_y(peer_acc)

    ratio = sigma[0] / alpha[0]
    base = noised.astype(F32) / alpha[0] - ratio * (resid.astype(F32) + own_acc)
    base = lax.optimization_barrier(base)
    denoised = base - ratio * recv.astype(F32)
    error = denoised - clean[0].astype(F32)
    total = jnp.sum(error * error) * weight[0] / (2 * rows * width)

    term = jnp.full((8, 128), total, F32)
    term = term + flip(term, CORE)
    plane = [term, flip(term, XBIT), flip_y(term)]
    corner = lax.ppermute(
        term, ("dp", "mp"), [(2 * i + j, 2 * (i ^ XBIT) + (1 - j)) for i in range(dp) for j in range(2)]
    )
    term = (plane[0] + plane[1]) + (plane[2] + corner)
    line = [term] + [flip(term, ZUNIT * k) for k in range(1, lines)]
    loss = functools.reduce(jnp.add, line)[0, 0]
    return denoised[None], loss


def make_adder(flat, piece):
    return jnp.einsum("rn,tnc->trc", flat, piece, preferred_element_type=jnp.float32)


def attend(operands):
    query_one, keys_one, values_one = operands
    rows = query_one.shape[0]
    total = keys_one.shape[0]
    scores = jnp.einsum(
        "qhd,khd->hqk",
        query_one.reshape(rows, HEADS, -1),
        keys_one.reshape(total, HEADS, -1),
        preferred_element_type=jnp.float32,
    ) * (query_one.shape[1] // HEADS) ** (-0.5)
    probs = jax.nn.softmax(scores, axis=-1).astype(jnp.bfloat16)
    mixed = jnp.einsum(
        "hqk,khd->qhd",
        probs,
        values_one.reshape(total, HEADS, -1),
        preferred_element_type=jnp.float32,
    )
    return mixed.astype(jnp.bfloat16).reshape(query_one.shape)


def plain_shards(
    clean,
    noise,
    tsteps,
    alpha_tab,
    weight_tab,
    norm1_gain,
    norm2_gain,
    wqkv,
    wout,
    wgate,
    wvalue,
    wdown,
):
    samples, local_rows, width = clean.shape
    alpha = lookup(tsteps, alpha_tab)
    sigma = jnp.sqrt(1.0 - alpha * alpha)
    weight = lookup(tsteps, weight_tab)
    noised = (
        alpha[:, None, None] * clean.astype(jnp.float32)
        + sigma[:, None, None] * noise.astype(jnp.float32)
    ).astype(jnp.bfloat16)
    normed1 = layer_norm(noised, norm1_gain)
    full_cols = lax.all_gather(wqkv, "mp", axis=2, tiled=True)
    flat = normed1.reshape(samples * local_rows, width)
    projected = make_adder(flat, lax.all_gather(full_cols, "dp", axis=1, tiled=True)).astype(
        jnp.bfloat16
    )
    query = projected[0].reshape(samples, local_rows, width)
    keys_part = projected[1].reshape(samples, local_rows, width)
    values_part = projected[2].reshape(samples, local_rows, width)
    keys_all, values_all = (
        lax.all_gather(keys_part, "mp", axis=1, tiled=True),
        lax.all_gather(values_part, "mp", axis=1, tiled=True),
    )
    mixed = lax.map(attend, (query, keys_all, values_all))
    mixed_flat = mixed.reshape(samples * local_rows, width)
    out_cols = lax.all_gather(wout, "mp", axis=1, tiled=True)
    part = mixed_flat
    projected_out = jnp.dot(
        part, lax.all_gather(out_cols, "dp", axis=0, tiled=True), preferred_element_type=jnp.float32
    )
    resid = (noised.astype(jnp.float32) + projected_out.reshape(samples, local_rows, width)).astype(
        jnp.bfloat16
    )
    normed2 = layer_norm(resid, norm2_gain)
    ff_in = lax.all_gather(normed2, "mp", axis=1, tiled=True)
    all_rows = ff_in.shape[1]
    ff_flat = ff_in.reshape(samples * all_rows, width)
    part = ff_flat
    gate = jnp.dot(
        part, lax.all_gather(wgate, "dp", axis=0, tiled=True), preferred_element_type=jnp.float32
    )
    value = jnp.dot(
        part, lax.all_gather(wvalue, "dp", axis=0, tiled=True), preferred_element_type=jnp.float32
    )
    hidden = (jax.nn.gelu(gate, approximate=False) * value).astype(jnp.bfloat16)
    block_sum = jnp.dot(
        hidden, lax.all_gather(wdown, "dp", axis=1, tiled=True), preferred_element_type=jnp.float32
    )
    ff_out = lax.psum_scatter(
        block_sum.reshape(samples, all_rows, width).astype(jnp.bfloat16),
        "mp",
        scatter_dimension=1,
        tiled=True,
    ).astype(jnp.float32)
    prediction = resid.astype(jnp.float32) + ff_out
    denoised = (noised.astype(jnp.float32) - sigma[:, None, None] * prediction) / alpha[
        :, None, None
    ]
    error = denoised - clean.astype(jnp.float32)
    local_terms = jnp.sum(weight * jnp.sum(error * error, axis=(1, 2))) / (all_rows * width)
    loss = lax.psum(local_terms, ("dp", "mp"))
    return (denoised, loss)


def solution(mesh):
    dp, mp = mesh.shape["dp"], mesh.shape["mp"]
    spec_w = P("dp", "mp")
    in_specs = (P("dp", "mp", None), P("dp", "mp", None), P("dp"), P(), P(), P(), P())
    in_specs += (P(None, "dp", "mp"), spec_w, spec_w, spec_w, P("mp", "dp"))
    out_specs = (P("dp", "mp", None), P())
    lines = dp // (SIDE * CORES)

    def run(*args):
        clean, wgate = args[0], args[9]
        hidden = wgate.shape[1] // (mp * CORES)
        width = clean.shape[2]
        fits = (
            mp == 2
            and clean.shape[0] == dp
            and lines * SIDE * CORES == dp
            and lines & (lines - 1) == 0
            and width == HEADS * HEAD_LANES
            and (width // mp) % 128 == 0
            and hidden % 256 == 0
            and (clean.shape[1] // mp) % 256 == 0
        )
        if fits:
            first = hidden * 2 // 5 // 256 * 256

            def body(*shards):
                return fast_shards(dp, (first, hidden - first), *shards)

        else:
            body = plain_shards
        step = jax.shard_map(body, mesh=mesh, in_specs=in_specs, out_specs=out_specs, check_vma=False)
        return step(*args)

    return run
```

```python
import functools

import jax
import jax.numpy as jnp
from jax import lax
from jax.experimental import pallas as pl
from jax.experimental.pallas import tpu as pltpu
from jax.sharding import PartitionSpec as P


HEADS = 20
EPS = 1e-05
CORES = 2
SIDE = 2
BF16 = jnp.bfloat16
F32 = jnp.float32
VMEM_LIMIT = 24 * 1024 * 1024


def lookup(steps, table):
    match = steps[:, None] == jnp.arange(table.shape[0], dtype=jnp.int32)[None, :]
    return jnp.sum(jnp.where(match, table[None, :], jnp.zeros((), table.dtype)), axis=1)


def layer_norm(values, gain):
    wide = values.astype(F32)
    center = wide - jnp.mean(wide, axis=-1, keepdims=True)
    spread = jnp.mean(center * center, axis=-1, keepdims=True)
    return (center * lax.rsqrt(spread + EPS) * gain).astype(BF16)


def dot(a, b):
    return jnp.dot(a, b, preferred_element_type=F32)


def dot_nt(a, b):
    return lax.dot_general(a, b, (((1,), (1,)), ((), ())), preferred_element_type=F32)


def hbm_spec():
    return pl.BlockSpec(memory_space=pltpu.HBM)


def vmem_spec():
    return pl.BlockSpec(memory_space=pltpu.VMEM)


def smem_spec():
    return pl.BlockSpec(memory_space=pltpu.SMEM)


def call(body, outs, in_specs, scratch, flops, nbytes, trans=0, out_specs=None):
    return pl.pallas_call(
        body,
        out_shape=outs,
        in_specs=in_specs,
        out_specs=out_specs if out_specs is not None else [vmem_spec() for _ in outs],
        scratch_shapes=scratch,
        compiler_params=pltpu.CompilerParams(vmem_limit_bytes=VMEM_LIMIT),
        cost_estimate=pl.CostEstimate(flops=flops, bytes_accessed=nbytes, transcendentals=trans),
    )


def piece_base(place, index, lines, rows):
    z, x = place[0], place[1]
    base = ((z ^ (index % lines)) * SIDE + (x ^ (index // lines))) * rows
    return pl.multiple_of(base, rows)


def attend_heads(q, k_ref, v_ref, pair, lane_low):
    k2 = k_ref[pair]
    v2 = v_ref[pair]
    halves = []
    for first in (True, False):
        keep = lane_low if first else jnp.logical_not(lane_low)
        qh = jnp.where(keep, q, jnp.zeros_like(q))
        s = dot_nt(qh, k2)
        m = jnp.max(s, axis=-1, keepdims=True)
        e = jnp.exp(s - m)
        total = jnp.sum(e, axis=-1, keepdims=True)
        o = dot(e.astype(BF16), v2)
        halves.append(o * (1.0 / total))
    return jnp.where(lane_low, halves[0], halves[1]).astype(BF16)


def attention_loop(q_ref, q_base, rows, k_ref, v_ref, out_ref, block):
    pairs = k_ref.shape[0]
    lane = lax.broadcasted_iota(jnp.int32, (block, 2 * HEAD_LANES), 1)
    lane_low = lane < HEAD_LANES

    def step(pair, carry):
        for t in range(rows // block):
            q = q_ref[pair, pl.ds(q_base + t * block, block), :]
            mixed = attend_heads(q, k_ref, v_ref, pair, lane_low)
            out_ref[pair, pl.ds(t * block, block), :] = mixed
        return carry

    lax.fori_loop(0, pairs, step, 0)


HEAD_LANES = 64


def qkv_body(scale, lines, place, n_own, n_peer, *refs):
    q_own, q_peer, k_out, v_out, w, sems = refs[4:]
    rows = refs[0].shape[1]
    pieces = refs[0].shape[0]

    def each(number, slot, act):
        for index in range(pieces):
            base = pl.ds(piece_base(place, index, lines, rows), rows)
            act(pltpu.make_async_copy(refs[number].at[index], w.at[slot, base, :], sems.at[slot]))

    for mat in range(2):
        for number in (mat, mat + 2):
            slot = (place[2] ^ (number // 2)) * 2 + mat

            @pl.when(slot < 3)
            def _(number=number, slot=slot):
                each(number, slot, lambda cp: cp.start())

    half = n_own.shape[0]
    block = 256
    pairs = k_out.shape[0]
    for mat in range(3):
        each(0, mat, lambda cp: cp.wait())
        for which, src in enumerate((n_own, n_peer)):
            for t in range(half // block):
                lo = t * block
                r = dot(src[lo : lo + block, :], w[mat]).astype(BF16)
                if mat == 0:
                    r = r * jnp.asarray(scale, BF16)
                for p in range(pairs):
                    col = r[:, p * 128 : (p + 1) * 128]
                    if mat == 0:
                        (q_own, q_peer)[which][p, lo : lo + block, :] = col
                    else:
                        at = which * half + lo
                        (k_out, v_out)[mat - 1][p, at : at + block, :] = col


def attn_body(q_ref, k_ref, v_ref, mixed_ref):
    attention_loop(q_ref, 0, q_ref.shape[1], k_ref, v_ref, mixed_ref, 256)


def wout_body(lines, place, gain, noised, m_own, m_peer, packed, second, y_own, y_partner, resid_ref, n2_ref, w, sems):
    rows = packed.shape[1]
    c = place[2]

    def run(sources, act):
        for index in range(packed.shape[0]):
            base = pl.ds(piece_base(place, index, lines, rows), rows)
            for slot, ref in enumerate(sources):
                act(pltpu.make_async_copy(ref.at[index], w.at[slot, base, :], sems.at[slot]))

    for act in (lambda cp: cp.start(), lambda cp: cp.wait()):

        @pl.when(c == 1)
        def _():
            run((packed, y_own), act)

        @pl.when(c == 0)
        def _():
            run((second, y_partner), act)

    y = place[3]
    pairs = m_own.shape[0]
    width = pairs * 128
    block = 256
    own0 = pl.multiple_of(y * width, width)
    peer0 = pl.multiple_of((1 - y) * width, width)
    for t in range(noised.shape[0] // block):
        sl = slice(t * block, (t + 1) * block)
        a_own = jnp.concatenate([m_own[p, sl, :] for p in range(pairs)], axis=-1)
        a_peer = jnp.concatenate([m_peer[p, sl, :] for p in range(pairs)], axis=-1)
        outs = []
        for h in range(2):
            outs.append(dot(a_own, w[h, pl.ds(own0, width), :]) + dot(a_peer, w[h, pl.ds(peer0, width), :]))
        first = jnp.where(y == 0, outs[0], outs[1])
        second = jnp.where(y == 0, outs[1], outs[0])
        out = jnp.concatenate([first, second], axis=-1)
        r = (noised[sl, :].astype(F32) + out).astype(BF16)
        resid_ref[sl, :] = r
        n2_ref[sl, :] = layer_norm(r, gain[...])


def ff_body(has_acc, first_row, groups, lines, place, x_ref, *refs):
    half = len(groups)
    stacks, rest = (refs[:half], refs[half : 2 * half]), refs[2 * half :]
    acc_in = None
    if has_acc:
        acc_in, rest = rest[0], rest[1:]
    *outs, w, sems = rest
    acc = outs.pop() if len(outs) == 2 else outs[0]
    taken = slice(first_row, first_row + acc.shape[0])
    rows = refs[0].shape[2]
    sub = w.shape[-1]
    n_sub = refs[0].shape[-1] // sub

    def each(c_flip, s, act):
        slot = c_flip * n_sub + s
        cols = pl.ds(pl.multiple_of(s * sub, sub), sub)
        for group, ref in zip(groups, stacks[c_flip]):
            for k, index in enumerate(group):
                base = pl.ds(piece_base(place, index, lines, rows), rows)
                act(pltpu.make_async_copy(ref.at[k, :, :, cols], w.at[slot, :, base, :], sems.at[slot]))

    for s in range(n_sub):
        each(0, s, lambda cp: cp.start())

    def product(slot):
        x = x_ref[taken, :]
        gate = dot(x, w[slot, 0])
        value = dot(x, w[slot, 1])
        hidden = (0.5 * gate * (1.0 + lax.erf(gate * (0.5**0.5))) * value).astype(BF16)
        return dot_nt(hidden, w[slot, 2])

    if has_acc:
        acc[...] = acc_in[taken, :]
    else:
        acc[...] = jnp.zeros_like(acc)
    for c_flip in range(CORES):

        def step(s, carry):
            if c_flip == 0:
                each(1, s, lambda cp: cp.start())
            each(c_flip, s, lambda cp: cp.wait())
            acc[...] += product(c_flip * n_sub + s)
            return carry

        lax.fori_loop(0, n_sub, step, 0)
    if outs and outs[0] is not acc:
        outs[0][...] = acc[...].astype(outs[0].dtype)


def fast_shards(dp, chunks, clean, noise, tsteps, alpha_tab, weight_tab, gain1, gain2, wqkv, wout, wgate, wvalue, wdown):
    _, rows, width = clean.shape
    heads_width = wout.shape[1]
    pairs = heads_width // 128
    lines = dp // (SIDE * CORES)
    me = lax.axis_index("dp")
    y = lax.axis_index("mp")
    c = me % CORES
    x = (me // CORES) % SIDE
    z = me // (CORES * SIDE)
    place = jnp.stack([z, x, c, y]).astype(jnp.int32)
    gain_row = gain2.reshape(1, width)

    def flip(value, bits):
        return lax.ppermute(value, "dp", [(i, i ^ bits) for i in range(dp)])

    def flip_y(value):
        return lax.ppermute(value, "mp", [(0, 1), (1, 0)])

    CORE, XBIT, ZUNIT = 1, CORES, CORES * SIDE

    b0 = jnp.concatenate([wqkv, wout[None]], axis=0)
    keep0 = lax.dynamic_slice_in_dim(b0, 2 * c, 2, 0)
    give0 = lax.dynamic_slice_in_dim(b0, 2 * (1 - c), 2, 0)
    first = c == 0

    def by_core(keep, recv):
        return jnp.concatenate([jnp.where(first, keep, recv), jnp.where(first, recv, keep)], axis=1)

    own0 = by_core(keep0, flip(give0, CORE))

    alpha = lookup(tsteps, alpha_tab)
    sigma = jnp.sqrt(1.0 - alpha * alpha)
    weight = lookup(tsteps, weight_tab)
    noised = (alpha[0] * clean[0].astype(F32) + sigma[0] * noise[0].astype(F32)).astype(BF16)
    n1 = layer_norm(noised, gain1)
    n1_peer = flip_y(n1)

    ffw = jnp.stack([wgate, wvalue, wdown.T])
    hidden_half = ffw.shape[2] // CORES
    keep_f = lax.dynamic_slice_in_dim(ffw, c * hidden_half, hidden_half, 2)
    give_f = lax.dynamic_slice_in_dim(ffw, (1 - c) * hidden_half, hidden_half, 2)
    recv_f = flip(give_f, CORE)

    def gather(own, late_by_z):
        zs, xs = [own], []
        for k in range(1, lines):
            top = 1 << (k.bit_length() - 1)
            if k == top:
                zs.append(flip(own, ZUNIT * k))
            else:
                zs.append(flip(zs[top], ZUNIT * (k - top)))
        for k in range(lines):
            top = 1 << max(k.bit_length() - 1, 0)
            if late_by_z and k == lines - 1 and k != top:
                xs.append(flip(xs[top], ZUNIT * (k - top)))
            else:
                xs.append(flip(zs[k], XBIT))
        return zs, xs

    def swap_packed(parts):
        packed = jnp.stack(parts)
        return packed, flip(packed, CORE)

    zs0, xs0 = gather(own0, False)
    mats = [swap_packed([p[m] for p in zs0 + xs0]) for m in range(2)]
    packed0, second0 = mats[1]

    half_shape = jax.ShapeDtypeStruct((pairs, rows, 128), BF16)
    full_shape = jax.ShapeDtypeStruct((pairs, 2 * rows, 128), BF16)
    wbytes = 4 * width * heads_width * 2
    scale = HEAD_LANES ** (-0.5)
    q_own, q_peer, k_all, v_all = call(
        functools.partial(qkv_body, scale, lines),
        [half_shape, half_shape, full_shape, full_shape],
        [smem_spec(), vmem_spec(), vmem_spec()] + [hbm_spec()] * 4,
        [
            pltpu.VMEM((3, width, heads_width), BF16),
            pltpu.SemaphoreType.DMA((3,)),
        ],
        8 * 10**9,
        wbytes + 8 * rows * width,
    )(place, n1, n1_peer, mats[0][0], packed0, mats[0][1], second0)

    def attend(q):
        return call(
            attn_body, [half_shape], [vmem_spec()] * 3, [], 12 * 10**9, 8 * rows * width
        )(q, k_all, v_all)[0]

    mixed_peer = attend(q_peer)
    m_recv = flip_y(mixed_peer)
    mixed_own = attend(q_own)

    y_own = lax.ppermute(
        packed0, ("dp", "mp"), [(2 * i + j, 2 * i + 1 - j) for i in range(1, dp, CORES) for j in range(2)]
    )
    y_partner = lax.ppermute(y_own, "dp", [(i, i - 1) for i in range(1, dp, CORES)])
    resid, n2 = call(
        functools.partial(wout_body, lines),
        [jax.ShapeDtypeStruct((rows, width), BF16)] * 2,
        [smem_spec()] + [vmem_spec()] * 4 + [hbm_spec()] * 4,
        [pltpu.VMEM((2, width, heads_width), BF16), pltpu.SemaphoreType.DMA((2,))],
        4 * 10**9,
        wbytes,
    )(place, gain_row, noised, mixed_own, m_recv, packed0, second0, y_own, y_partner)
    n2_peer = flip_y(n2)

    def ff(tokens, first_row, t, groups, stacks, hc, sub, acc, out_dtype):
        n_sub = hc // sub
        args = [place, tokens, *stacks]
        specs = [smem_spec(), vmem_spec()] + [hbm_spec()] * len(stacks)
        if acc is not None:
            args.append(acc)
            specs.append(vmem_spec())
        return call(
            functools.partial(ff_body, acc is not None, first_row, groups, lines),
            [jax.ShapeDtypeStruct((t, width), out_dtype)],
            specs,
            ([pltpu.VMEM((t, width), F32)] if out_dtype != F32 else [])
            + [
                pltpu.VMEM((CORES * n_sub, 3, width, sub), BF16),
                pltpu.SemaphoreType.DMA((CORES * n_sub,)),
            ],
            2 * t * width * hc * 2 * 3,
            3 * width * hc * 4,
        )(*args)[0]

    peer_acc = own_acc = None
    start = 0
    for index, hc in enumerate(chunks):
        sub = 256 if hc % 256 == 0 else 128
        part = slice(start, start + hc)
        zs, xs = gather(by_core(keep_f[:, :, part], recv_f[:, :, part]), index > 0)
        pieces = zs + xs
        groups = [tuple(range(lines)), tuple(range(lines, 2 * lines, 2))]
        groups += [(n,) for n in range(lines + 1, 2 * lines, 2)]
        stacks = []
        for group in groups:
            if len(group) > 1:
                stacks.append(swap_packed([pieces[n] for n in group]))
            else:
                piece = pieces[group[0]]
                stacks.append((piece[None], flip(piece, CORE)[None]))
        stacks = [pair[n] for n in range(2) for pair in stacks]
        last = index == len(chunks) - 1
        if last:
            half = rows // 2
            parts = [
                ff(n2_peer, n * half, half, groups, stacks, hc, sub, peer_acc, BF16)
                for n in range(2)
            ]
        else:
            peer_acc = ff(n2_peer, 0, rows, groups, stacks, hc, sub, peer_acc, F32)
        own_acc = ff(n2, 0, rows, groups, stacks, hc, sub, own_acc, F32)
        start += hc
    recv = jnp.concatenate([flip_y(part) for part in parts])

    ratio = sigma[0] / alpha[0]
    base = noised.astype(F32) / alpha[0] - ratio * (resid.astype(F32) + own_acc)
    base = lax.optimization_barrier(base)
    denoised = base - ratio * recv.astype(F32)
    error = denoised - clean[0].astype(F32)
    total = jnp.sum(error * error) * weight[0] / (2 * rows * width)

    term = jnp.full((8, 128), total, F32)
    term = term + flip(term, CORE)
    plane = [term, flip(term, XBIT), flip_y(term)]
    corner = lax.ppermute(
        term, ("dp", "mp"), [(2 * i + j, 2 * (i ^ XBIT) + (1 - j)) for i in range(dp) for j in range(2)]
    )
    term = (plane[0] + plane[1]) + (plane[2] + corner)
    line = [term] + [flip(term, ZUNIT * k) for k in range(1, lines)]
    loss = functools.reduce(jnp.add, line)[0, 0]
    return denoised[None], loss


def make_adder(flat, piece):
    return jnp.einsum("rn,tnc->trc", flat, piece, preferred_element_type=jnp.float32)


def attend(operands):
    query_one, keys_one, values_one = operands
    rows = query_one.shape[0]
    total = keys_one.shape[0]
    scores = jnp.einsum(
        "qhd,khd->hqk",
        query_one.reshape(rows, HEADS, -1),
        keys_one.reshape(total, HEADS, -1),
        preferred_element_type=jnp.float32,
    ) * (query_one.shape[1] // HEADS) ** (-0.5)
    probs = jax.nn.softmax(scores, axis=-1).astype(jnp.bfloat16)
    mixed = jnp.einsum(
        "hqk,khd->qhd",
        probs,
        values_one.reshape(total, HEADS, -1),
        preferred_element_type=jnp.float32,
    )
    return mixed.astype(jnp.bfloat16).reshape(query_one.shape)


def plain_shards(
    clean,
    noise,
    tsteps,
    alpha_tab,
    weight_tab,
    norm1_gain,
    norm2_gain,
    wqkv,
    wout,
    wgate,
    wvalue,
    wdown,
):
    samples, local_rows, width = clean.shape
    alpha = lookup(tsteps, alpha_tab)
    sigma = jnp.sqrt(1.0 - alpha * alpha)
    weight = lookup(tsteps, weight_tab)
    noised = (
        alpha[:, None, None] * clean.astype(jnp.float32)
        + sigma[:, None, None] * noise.astype(jnp.float32)
    ).astype(jnp.bfloat16)
    normed1 = layer_norm(noised, norm1_gain)
    full_cols = lax.all_gather(wqkv, "mp", axis=2, tiled=True)
    flat = normed1.reshape(samples * local_rows, width)
    projected = make_adder(flat, lax.all_gather(full_cols, "dp", axis=1, tiled=True)).astype(
        jnp.bfloat16
    )
    query = projected[0].reshape(samples, local_rows, width)
    keys_part = projected[1].reshape(samples, local_rows, width)
    values_part = projected[2].reshape(samples, local_rows, width)
    keys_all, values_all = (
        lax.all_gather(keys_part, "mp", axis=1, tiled=True),
        lax.all_gather(values_part, "mp", axis=1, tiled=True),
    )
    mixed = lax.map(attend, (query, keys_all, values_all))
    mixed_flat = mixed.reshape(samples * local_rows, width)
    out_cols = lax.all_gather(wout, "mp", axis=1, tiled=True)
    part = mixed_flat
    projected_out = jnp.dot(
        part, lax.all_gather(out_cols, "dp", axis=0, tiled=True), preferred_element_type=jnp.float32
    )
    resid = (noised.astype(jnp.float32) + projected_out.reshape(samples, local_rows, width)).astype(
        jnp.bfloat16
    )
    normed2 = layer_norm(resid, norm2_gain)
    ff_in = lax.all_gather(normed2, "mp", axis=1, tiled=True)
    all_rows = ff_in.shape[1]
    ff_flat = ff_in.reshape(samples * all_rows, width)
    part = ff_flat
    gate = jnp.dot(
        part, lax.all_gather(wgate, "dp", axis=0, tiled=True), preferred_element_type=jnp.float32
    )
    value = jnp.dot(
        part, lax.all_gather(wvalue, "dp", axis=0, tiled=True), preferred_element_type=jnp.float32
    )
    hidden = (jax.nn.gelu(gate, approximate=False) * value).astype(jnp.bfloat16)
    block_sum = jnp.dot(
        hidden, lax.all_gather(wdown, "dp", axis=1, tiled=True), preferred_element_type=jnp.float32
    )
    ff_out = lax.psum_scatter(
        block_sum.reshape(samples, all_rows, width).astype(jnp.bfloat16),
        "mp",
        scatter_dimension=1,
        tiled=True,
    ).astype(jnp.float32)
    prediction = resid.astype(jnp.float32) + ff_out
    denoised = (noised.astype(jnp.float32) - sigma[:, None, None] * prediction) / alpha[
        :, None, None
    ]
    error = denoised - clean.astype(jnp.float32)
    local_terms = jnp.sum(weight * jnp.sum(error * error, axis=(1, 2))) / (all_rows * width)
    loss = lax.psum(local_terms, ("dp", "mp"))
    return (denoised, loss)


def solution(mesh):
    dp, mp = mesh.shape["dp"], mesh.shape["mp"]
    spec_w = P("dp", "mp")
    in_specs = (P("dp", "mp", None), P("dp", "mp", None), P("dp"), P(), P(), P(), P())
    in_specs += (P(None, "dp", "mp"), spec_w, spec_w, spec_w, P("mp", "dp"))
    out_specs = (P("dp", "mp", None), P())
    lines = dp // (SIDE * CORES)

    def run(*args):
        clean, wgate = args[0], args[9]
        hidden = wgate.shape[1] // (mp * CORES)
        width = clean.shape[2]
        fits = (
            mp == 2
            and clean.shape[0] == dp
            and lines * SIDE * CORES == dp
            and lines & (lines - 1) == 0
            and width == HEADS * HEAD_LANES
            and (width // mp) % 128 == 0
            and hidden % 256 == 0
            and (clean.shape[1] // mp) % 256 == 0
        )
        if fits:
            first = hidden * 2 // 5 // 256 * 256

            def body(*shards):
                return fast_shards(dp, (first, hidden - first), *shards)

        else:
            body = plain_shards
        step = jax.shard_map(body, mesh=mesh, in_specs=in_specs, out_specs=out_specs, check_vma=False)
        return step(*args)

    return run
```
